32 devices in a mesh: tm: 16 (over z, x, core), mom: 2 (over y).
Axes of the slice: x: 2, y: 2, z: 4, core: 2. Of those that a mesh axis runs over, the one named last changes fastest.
Arguments:
- fields: bfloat16 [16, 4, 2, 512, 512], P('tm', 'mom'), may hold values from -1 to 1
- mom_pairs: int32 [6, 2], P('mom'), may hold values from 0 to 3, as said below
- deltas: int32 [4], replicated, may hold values from 0 to 3, each once
Outputs:
- time_traces: float32 [16, 2, 4, 6], P('tm', None, None, 'mom')
- summed_traces: float32 [2, 4, 6], P(None, None, 'mom')
The draws below stay inside these ranges and needn't reach their ends.
Inputs may be any that keep to these rules, and one draw needn't show every extreme that they name: `mom_pairs`: column 0 may be any momentum; in row r, column 1 lies in momentum group r // 3, that is from (r // 3) * 2 to (r // 3) * 2 + 1.
All inputs are finite; a program needn't handle non-finite values.
Results may differ from the reference program's by a relative error of at most 0.0003.
Values may be sent and summed in bfloat16 or wider, within the bound.
A program may use at most 128 MiB of HBM per device.

```python
import jax
import jax.numpy as jnp
from jax import lax

NEV = 512
PG = 2
PAIR_DEV = 3
NSEP = 4
P_SIZE = 4
NPAIR = 6
NT = 16


def draw_fields(key, part):
    field_shape = (NT, P_SIZE, 2, NEV, NEV)
    key_base = jax.random.fold_in(jax.random.fold_in(key, 11), 0)
    growth = jnp.sqrt(3.0) ** (jnp.arange(NT, dtype=jnp.float32) / max(NT - 1, 1))
    values = jax.random.normal(key_base, field_shape, jnp.float32)
    values = values * growth[:, None, None, None, None] / jnp.sqrt(jnp.float32(NEV))
    return jnp.clip(values, -1.0, 1.0).astype(jnp.bfloat16)


def draw_mom_pairs(key, part):
    key_source, key_target = jax.random.split(jax.random.fold_in(key, 23), 2)
    source_mom = jax.random.randint(key_source, (NPAIR,), 0, P_SIZE)
    owner = jnp.arange(NPAIR, dtype=jnp.int32) // PAIR_DEV
    target_mom = owner * PG + jax.random.randint(key_target, (NPAIR,), 0, PG)
    return jnp.stack([source_mom, target_mom], axis=1).astype(jnp.int32)


def setup_inputs(seed: int = 0) -> dict:
    streams_of = jax.random.split(jax.random.key(seed), 4)
    fields = draw_fields(jax.random.fold_in(streams_of[3], 71), 0)
    mom_pairs = draw_mom_pairs(jax.random.fold_in(streams_of[3], 71), 0)
    deltas = jax.random.permutation(streams_of[2], NSEP).astype(jnp.int32)
    return dict(fields=fields, mom_pairs=mom_pairs, deltas=deltas)


def products(source, target):
    product_full = jnp.einsum("xij,yjk->xyik", source.astype(jnp.float32), target.astype(jnp.float32))
    real_part = product_full[0, 0] - product_full[1, 1]
    imag_part = product_full[0, 1] + product_full[1, 0]
    direct = jnp.trace(real_part)
    box_value = jnp.sum(real_part * real_part.T) - jnp.sum(imag_part * imag_part.T)
    return direct, box_value


def reference(fields, mom_pairs, deltas):
    slices = fields.shape[0]
    pair_count = mom_pairs.shape[0]

    def one_time(time_slice):
        source_slice = lax.dynamic_index_in_dim(fields, time_slice, 0, keepdims=False)
        per_sep = []
        for separation in range(1, NSEP + 1):
            later = ((time_slice + separation) % slices).astype(jnp.int32)
            target_slice = lax.dynamic_index_in_dim(fields, later, 0, keepdims=False)
            directs = []
            boxes = []
            for which in range(pair_count):
                source = lax.dynamic_index_in_dim(source_slice, mom_pairs[which, 0].astype(jnp.int32), 0, keepdims=False)
                target = lax.dynamic_index_in_dim(target_slice, mom_pairs[which, 1].astype(jnp.int32), 0, keepdims=False)
                direct, box_value = products(source, target)
                directs.append(direct)
                boxes.append(box_value)
            per_sep.append(jnp.stack([jnp.stack(directs), jnp.stack(boxes)]))
        return jnp.stack(per_sep, axis=1)

    stacked = lax.map(one_time, jnp.arange(slices, dtype=jnp.int32))
    time_traces = jnp.take(stacked, deltas.astype(jnp.int32), axis=2)
    summed_traces = jnp.sum(time_traces, axis=0)
    return time_traces, summed_traces
```

```python
import functools

import jax
import jax.numpy as jnp
from jax import lax
from jax.experimental import pallas as pl
from jax.experimental.pallas import tpu as pltpu
from jax.sharding import PartitionSpec as P

MESH = pl.DeviceIdType.MESH
BLK = 128


def kernel(n_tm, n_mom, pair_ref, field_ref, local_ref, sum_ref, *scratch):
    per_group, _, nev, _ = field_ref.shape[1:]
    stages = nev // BLK
    slots = 4
    subs = per_group * 2
    pairs = pair_ref.shape[0]
    a_bufs = scratch[:stages]
    b_flat = scratch[stages : stages + stages * slots]
    b_bufs = [b_flat[n * slots : (n + 1) * slots] for n in range(stages)]
    acc_d, acc_b, gathered = scratch[stages + stages * slots : stages + stages * slots + 3]
    own_sem, y_send, y_recv, b_send, b_recv, r_send, r_recv = scratch[-7:]

    me = lax.axis_index("tm")
    group = lax.axis_index("mom")

    def at(step):
        return {"tm": lax.rem(me + step + n_tm, n_tm), "mom": group}

    upper_core = lax.rem(me, 2) == 1
    odd_chip = lax.rem(me // 2, 2) == 1

    own_copies = []
    for n in range(stages):
        copy = pltpu.make_async_copy(
            field_ref.at[0, :, :, pl.ds(n * BLK, BLK), :],
            a_bufs[n].at[pl.ds(group * per_group, per_group)],
            own_sem.at[n],
        )
        copy.start()
        own_copies.append(copy)

    barrier = pltpu.get_barrier_semaphore()

    def greet(i, carry):
        pl.semaphore_signal(barrier, inc=1, device_id=at(i), device_id_type=MESH)
        return carry

    lax.fori_loop(1, n_tm, greet, 0)
    for j in range(1, n_mom):
        pl.semaphore_signal(
            barrier, inc=1, device_id={"tm": me, "mom": lax.rem(group + j, n_mom)}, device_id_type=MESH
        )
    pl.semaphore_wait(barrier, n_tm - 1 + n_mom - 1)

    def own_part(n, sub):
        return field_ref.at[0, sub // 2, sub % 2, :, pl.ds(n * BLK, BLK)]

    def part(n, slot, sub):
        return b_bufs[n][slot - 1].at[sub // 2, sub % 2]

    def hop(src, n, slot, sub, step):
        return pltpu.make_async_remote_copy(
            src_ref=src,
            dst_ref=part(n, slot, sub),
            send_sem=b_send.at[slot - 1, n, sub],
            recv_sem=b_recv.at[slot - 1, n, sub],
            device_id=at(step),
            device_id_type=MESH,
        )

    def across(n, j):
        return pltpu.make_async_remote_copy(
            src_ref=field_ref.at[0, :, :, pl.ds(n * BLK, BLK), :],
            dst_ref=a_bufs[n].at[pl.ds(group * per_group, per_group)],
            send_sem=y_send.at[n, j],
            recv_sem=y_recv.at[n, j],
            device_id={"tm": me, "mom": lax.rem(group + j, n_mom)},
            device_id_type=MESH,
        )

    for n in range(stages):
        for j in range(1, n_mom):
            across(n, j).start()
        for sub in range(subs):
            hop(own_part(n, sub), n, 4, sub, -4).start()

        @pl.when(odd_chip)
        def _():
            for sub in range(subs):
                hop(own_part(n, sub), n, 2, sub, -2).start()

        @pl.when(upper_core)
        def _():
            for sub in range(subs):
                hop(own_part(n, sub), n, 1, sub, -1).start()

    def relay(n, sub):
        hop(part(n, 4, sub), n, 4, sub, -4).wait_recv()

        @pl.when(jnp.logical_not(odd_chip))
        def _():
            hop(part(n, 4, sub), n, 2, sub, 2).start()

        @pl.when(jnp.logical_not(upper_core))
        def _():
            hop(part(n, 4, sub), n, 3, sub, 1).start()

        hop(part(n, 2, sub), n, 2, sub, -2).wait_recv()

        @pl.when(upper_core)
        def _():
            hop(part(n, 2, sub), n, 3, sub, -1).start()

        @pl.when(jnp.logical_not(upper_core))
        def _():
            hop(part(n, 2, sub), n, 1, sub, 1).start()

    acc_d[...] = jnp.zeros_like(acc_d)
    acc_b[...] = jnp.zeros_like(acc_b)
    eye = (
        lax.broadcasted_iota(jnp.int32, (BLK, BLK), 0) == lax.broadcasted_iota(jnp.int32, (BLK, BLK), 1)
    ).astype(jnp.float32)

    def fold(x):
        return jnp.sum(x.reshape(BLK // 8, 8, BLK), axis=0)

    def compute(n, slot):
        def body(k, carry):
            a = pair_ref[k, 0]
            b = lax.rem(pair_ref[k, 1], per_group)

            def left(i):
                return jnp.concatenate([a_bufs[i][a, 0], a_bufs[i][a, 1]], axis=1)

            def right(i):
                buf = b_bufs[i][slot - 1]
                re, im = buf[b, 0], buf[b, 1]
                return jnp.concatenate(
                    [jnp.concatenate([re, im], axis=1), jnp.concatenate([-im, re], axis=1)], axis=0
                )

            lhs = left(n)
            column = jnp.dot(
                jnp.concatenate([left(i) for i in range(n)] + [lhs], axis=0),
                right(n),
                preferred_element_type=jnp.float32,
            )
            box = jnp.zeros((BLK, BLK), jnp.float32)
            for j in range(n):
                row = jnp.dot(lhs, right(j), preferred_element_type=jnp.float32)
                upper = column[j * BLK : (j + 1) * BLK]
                box += upper[:, :BLK] * row[:, :BLK].T - upper[:, BLK:] * row[:, BLK:].T
            corner = column[n * BLK :]
            re, im = corner[:, :BLK], corner[:, BLK:]
            box = box + box + re * re.T - im * im.T
            index = (slot - 1) * pairs + k
            acc_b[index] += fold(box)
            acc_d[index] += fold(re * eye)
            return carry

        lax.fori_loop(0, pairs, body, 0)

    for sub in range(subs):
        relay(0, sub)
    for n in range(stages):
        own_copies[n].wait()
        for j in range(1, n_mom):
            across(n, j).wait_recv()
        for place, slot in enumerate((4, 2, 1, 3)):
            if slot % 2 == 1:
                for sub in range(subs):
                    hop(part(n, slot, sub), n, slot, sub, -1).wait_recv()
            compute(n, slot)
            if n + 1 < stages:
                for sub in range(place * subs // slots, (place + 1) * subs // slots):
                    relay(n + 1, sub)

    def lanes(acc):
        count = acc.shape[0]
        each = jnp.sum(jnp.sum(acc[...], axis=1), axis=1, keepdims=True)
        row = lax.broadcasted_iota(jnp.int32, (count, BLK), 0)
        lane = lax.broadcasted_iota(jnp.int32, (count, BLK), 1)
        return jnp.sum(jnp.where(row == lane, jnp.broadcast_to(each, (count, BLK)), 0.0), axis=0, keepdims=True)

    which = lax.broadcasted_iota(jnp.int32, (8, BLK), 0)
    stat = jnp.where(which == 0, lanes(acc_d), jnp.where(which == 1, lanes(acc_b), 0.0))
    gathered[me] = stat
    local_ref[...] = stat

    def give(i):
        return pltpu.make_async_remote_copy(
            src_ref=gathered.at[me],
            dst_ref=gathered.at[me],
            send_sem=r_send.at[i],
            recv_sem=r_recv.at[i],
            device_id=at(i),
            device_id_type=MESH,
        )

    def start_give(i, carry):
        give(i).start()
        return carry

    lax.fori_loop(1, n_tm, start_give, 0)
    for n in range(stages):
        for j in range(1, n_mom):
            across(n, j).wait_send()
        for sub in range(subs):
            for slot in range(1, slots + 1):
                hop(part(n, slot, sub), n, slot, sub, -1).wait_send()

    def end_give(i, carry):
        give(i).wait()
        return carry

    lax.fori_loop(1, n_tm, end_give, 0)
    sum_ref[...] = jnp.sum(gathered[...], axis=0)


def reorder(stacked, deltas):
    picker = (deltas[:, None] == jnp.arange(deltas.shape[0], dtype=jnp.int32)[None, :]).astype(
        jnp.float32
    )
    return jnp.sum(picker[:, :, None] * stacked[..., None, :, :], axis=-2)


def per_device(n_tm, n_mom, fields, mom_pairs, deltas):
    _, per_group, _, nev, _ = fields.shape
    pairs = mom_pairs.shape[0]
    seps = deltas.shape[0]
    stages = nev // BLK
    subs = per_group * 2
    slots = 4
    rows = -(-seps * pairs // 8) * 8
    scratch = (
        [pltpu.VMEM((n_mom * per_group, 2, BLK, nev), fields.dtype)] * stages
        + [pltpu.VMEM((per_group, 2, nev, BLK), fields.dtype)] * (stages * slots)
        + [pltpu.VMEM((rows, 8, BLK), jnp.float32)] * 2
        + [pltpu.VMEM((n_tm, 8, BLK), jnp.float32)]
        + [
            pltpu.SemaphoreType.DMA((stages,)),
            pltpu.SemaphoreType.DMA((stages, n_mom)),
            pltpu.SemaphoreType.DMA((stages, n_mom)),
            pltpu.SemaphoreType.DMA((slots, stages, subs)),
            pltpu.SemaphoreType.DMA((slots, stages, subs)),
            pltpu.SemaphoreType.DMA((n_tm,)),
            pltpu.SemaphoreType.DMA((n_tm,)),
        ]
    )
    tile = jax.ShapeDtypeStruct((8, BLK), jnp.float32)
    local, total = pl.pallas_call(
        functools.partial(kernel, n_tm, n_mom),
        out_shape=(tile, tile),
        in_specs=[pl.BlockSpec(memory_space=pltpu.SMEM), pl.BlockSpec(memory_space=pl.ANY)],
        out_specs=(pl.BlockSpec(memory_space=pltpu.VMEM), pl.BlockSpec(memory_space=pltpu.VMEM)),
        scratch_shapes=scratch,
        compiler_params=pltpu.CompilerParams(
            collective_id=0, has_side_effects=True, vmem_limit_bytes=48 * 1024 * 1024
        ),
    )(mom_pairs, fields)

    def unpack(x):
        return reorder(x[:2, : seps * pairs].reshape(2, seps, pairs), deltas)

    return (unpack(local)[None], unpack(total))


def solution(mesh):
    return jax.shard_map(
        functools.partial(per_device, mesh.shape["tm"], mesh.shape["mom"]),
        mesh=mesh,
        in_specs=(P("tm", "mom", None, None, None), P("mom", None), P()),
        out_specs=(P("tm", None, None, "mom"), P(None, None, "mom")),
        check_vma=False,
    )
```

```python
import functools

import jax
import jax.numpy as jnp
from jax import lax
from jax.experimental import pallas as pl
from jax.experimental.pallas import tpu as pltpu
from jax.sharding import PartitionSpec as P

MESH = pl.DeviceIdType.MESH
BLK = 128


def kernel(n_tm, n_mom, pair_ref, delta_ref, field_ref, local_ref, sum_ref, *scratch):
    per_group, _, nev, _ = field_ref.shape[1:]
    stages = nev // BLK
    slots = 4
    subs = per_group * 2
    pairs = pair_ref.shape[1]
    seps = delta_ref.shape[0]
    a_bufs = scratch[:stages]
    b_flat = scratch[stages : stages + stages * slots]
    b_bufs = [b_flat[n * slots : (n + 1) * slots] for n in range(stages)]
    acc_d, acc_b, held, gathered = scratch[stages + stages * slots : stages + stages * slots + 4]
    own_sem, y_send, y_recv, b_send, b_recv, r_send, r_recv = scratch[-7:]

    me = lax.axis_index("tm")
    group = lax.axis_index("mom")

    def at(step):
        return {"tm": lax.rem(me + step + n_tm, n_tm), "mom": group}

    upper_core = lax.rem(me, 2) == 1
    odd_chip = lax.rem(me // 2, 2) == 1

    own_copies = []
    for n in range(stages):
        copy = pltpu.make_async_copy(
            field_ref.at[0, :, :, pl.ds(n * BLK, BLK), :],
            a_bufs[n].at[pl.ds(group * per_group, per_group)],
            own_sem.at[n],
        )
        copy.start()
        own_copies.append(copy)

    barrier = pltpu.get_barrier_semaphore()

    def greet(i, carry):
        pl.semaphore_signal(barrier, inc=1, device_id=at(i), device_id_type=MESH)
        return carry

    lax.fori_loop(1, n_tm, greet, 0)
    for j in range(1, n_mom):
        pl.semaphore_signal(
            barrier, inc=1, device_id={"tm": me, "mom": lax.rem(group + j, n_mom)}, device_id_type=MESH
        )
    pl.semaphore_wait(barrier, n_tm - 1 + n_mom - 1)

    def own_part(n, sub):
        return field_ref.at[0, sub // 2, sub % 2, :, pl.ds(n * BLK, BLK)]

    def part(n, slot, sub):
        return b_bufs[n][slot - 1].at[sub // 2, sub % 2]

    def hop(src, n, slot, sub, step):
        return pltpu.make_async_remote_copy(
            src_ref=src,
            dst_ref=part(n, slot, sub),
            send_sem=b_send.at[slot - 1, n, sub],
            recv_sem=b_recv.at[slot - 1, n, sub],
            device_id=at(step),
            device_id_type=MESH,
        )

    def across(n, j):
        return pltpu.make_async_remote_copy(
            src_ref=field_ref.at[0, :, :, pl.ds(n * BLK, BLK), :],
            dst_ref=a_bufs[n].at[pl.ds(group * per_group, per_group)],
            send_sem=y_send.at[n, j],
            recv_sem=y_recv.at[n, j],
            device_id={"tm": me, "mom": lax.rem(group + j, n_mom)},
            device_id_type=MESH,
        )

    for n in range(stages):
        for j in range(1, n_mom):
            across(n, j).start()
        for sub in range(subs):
            hop(own_part(n, sub), n, 4, sub, -4).start()

        @pl.when(odd_chip)
        def _():
            for sub in range(subs):
                hop(own_part(n, sub), n, 2, sub, -2).start()

        @pl.when(upper_core)
        def _():
            for sub in range(subs):
                hop(own_part(n, sub), n, 1, sub, -1).start()

    def relay_four(n, sub):
        hop(part(n, 4, sub), n, 4, sub, -4).wait_recv()

        @pl.when(jnp.logical_not(odd_chip))
        def _():
            hop(part(n, 4, sub), n, 2, sub, 2).start()

        @pl.when(jnp.logical_not(upper_core))
        def _():
            hop(part(n, 4, sub), n, 3, sub, 1).start()

    def relay_two(n, sub):
        hop(part(n, 2, sub), n, 2, sub, -2).wait_recv()

        @pl.when(upper_core)
        def _():
            hop(part(n, 2, sub), n, 3, sub, -1).start()

        @pl.when(jnp.logical_not(upper_core))
        def _():
            hop(part(n, 2, sub), n, 1, sub, 1).start()

    acc_d[...] = jnp.zeros_like(acc_d)
    acc_b[...] = jnp.zeros_like(acc_b)
    eye = (
        lax.broadcasted_iota(jnp.int32, (BLK, BLK), 0) == lax.broadcasted_iota(jnp.int32, (BLK, BLK), 1)
    ).astype(jnp.float32)

    def fold(x):
        return jnp.sum(x.reshape(BLK // 8, 8, BLK), axis=0)

    def left(i, k):
        a = pair_ref[0, k]
        return jnp.concatenate([a_bufs[i][a, 0], a_bufs[i][a, 1]], axis=1)

    def right(i, slot, k):
        b = lax.rem(pair_ref[1, k], per_group)
        buf = b_bufs[i][slot - 1]
        re, im = buf[b, 0], buf[b, 1]
        return jnp.concatenate(
            [jnp.concatenate([re, im], axis=1), jnp.concatenate([-im, re], axis=1)], axis=0
        )

    def rows_of(n, slot):
        for k in range(pairs):
            lhs = left(n, k)
            for j in range(n):
                row = jnp.dot(lhs, right(j, slot, k), preferred_element_type=jnp.float32)
                index = (slot - 1) * pairs + k
                held[index, j, 0] = row[:, :BLK].T
                held[index, j, 1] = row[:, BLK:].T

    def columns_of(n, slot):
        for k in range(pairs):
            index = (slot - 1) * pairs + k
            column = jnp.dot(
                jnp.concatenate([left(i, k) for i in range(n + 1)], axis=0),
                right(n, slot, k),
                preferred_element_type=jnp.float32,
            )
            box = jnp.zeros((BLK, BLK), jnp.float32)
            for j in range(n):
                upper = column[j * BLK : (j + 1) * BLK]
                box += upper[:, :BLK] * held[index, j, 0] - upper[:, BLK:] * held[index, j, 1]
            corner = column[n * BLK :]
            re, im = corner[:, :BLK], corner[:, BLK:]
            box = box + box + re * re.T - im * im.T
            acc_b[index] += fold(box)
            acc_d[index] += fold(re * eye)

    order = (4, 2, 1, 3)
    share = [range(p * subs // slots, (p + 1) * subs // slots) for p in range(slots)]
    late = share[-1]
    for sub in range(subs):
        relay_four(0, sub)
        relay_two(0, sub)
    for n in range(stages):
        own_copies[n].wait()
        for j in range(1, n_mom):
            across(n, j).wait_recv()
        if n:
            for slot in order[: slots // 2]:
                rows_of(n, slot)
            for sub in late:
                relay_two(n, sub)
            for slot in order[slots // 2 :]:
                rows_of(n, slot)
        for place, slot in enumerate(order):
            if slot % 2 == 1:
                for sub in range(subs):
                    hop(part(n, slot, sub), n, slot, sub, -1).wait_recv()
            columns_of(n, slot)
            if n + 1 < stages:
                for sub in share[place]:
                    relay_four(n + 1, sub)
                    if place < slots - 1:
                        relay_two(n + 1, sub)

    count = acc_d.shape[0]
    height = gathered.shape[1]
    lane = lax.broadcasted_iota(jnp.int32, (1, BLK), 1)
    wanted = jnp.zeros((1, BLK), jnp.int32)
    for r in range(seps):
        wanted = jnp.where(lane == r, delta_ref[r], wanted)
    index = lax.broadcasted_iota(jnp.int32, (count, BLK), 0)
    which = lax.broadcasted_iota(jnp.int32, (height, BLK), 0)
    stat = jnp.zeros((height, BLK), jnp.float32)
    for p, acc in enumerate((acc_d, acc_b)):
        each = jnp.sum(jnp.sum(acc[...], axis=1), axis=1, keepdims=True)
        each = jnp.broadcast_to(each, (count, BLK))
        for k in range(pairs):
            line = jnp.sum(jnp.where(index == wanted * pairs + k, each, 0.0), axis=0, keepdims=True)
            stat = jnp.where(which == 2 * k + p, jnp.broadcast_to(line, (height, BLK)), stat)
    gathered[me] = stat

    def write(ref, value):
        for k in range(pairs):
            ref[k] = value[2 * k : 2 * k + 2, :seps]

    def give(i):
        return pltpu.make_async_remote_copy(
            src_ref=gathered.at[me],
            dst_ref=gathered.at[me],
            send_sem=r_send.at[i],
            recv_sem=r_recv.at[i],
            device_id=at(i),
            device_id_type=MESH,
        )

    far = sorted(range(1, n_tm), key=lambda i: -min(i, n_tm - i))
    for i in far:
        give(i).start()
    write(local_ref, stat)
    for n in range(stages):
        for j in range(1, n_mom):
            across(n, j).wait_send()
        for sub in range(subs):
            for slot in range(1, slots + 1):
                hop(part(n, slot, sub), n, slot, sub, -1).wait_send()

    for i in reversed(far):
        give(i).wait()
    write(sum_ref, jnp.sum(gathered[...], axis=0))


def per_device(n_tm, n_mom, fields, mom_pairs, deltas):
    _, per_group, _, nev, _ = fields.shape
    pairs = mom_pairs.shape[0]
    seps = deltas.shape[0]
    stages = nev // BLK
    subs = per_group * 2
    slots = 4
    rows = -(-seps * pairs // 8) * 8
    height = -(-2 * pairs // 8) * 8
    scratch = (
        [pltpu.VMEM((n_mom * per_group, 2, BLK, nev), fields.dtype)] * stages
        + [pltpu.VMEM((per_group, 2, nev, BLK), fields.dtype)] * (stages * slots)
        + [pltpu.VMEM((rows, 8, BLK), jnp.float32)] * 2
        + [pltpu.VMEM((rows, stages - 1, 2, BLK, BLK), jnp.float32)]
        + [pltpu.VMEM((n_tm, height, BLK), jnp.float32)]
        + [
            pltpu.SemaphoreType.DMA((stages,)),
            pltpu.SemaphoreType.DMA((stages, n_mom)),
            pltpu.SemaphoreType.DMA((stages, n_mom)),
            pltpu.SemaphoreType.DMA((slots, stages, subs)),
            pltpu.SemaphoreType.DMA((slots, stages, subs)),
            pltpu.SemaphoreType.DMA((n_tm,)),
            pltpu.SemaphoreType.DMA((n_tm,)),
        ]
    )
    tile = jax.ShapeDtypeStruct((pairs, 2, seps), jnp.float32)
    local, total = pl.pallas_call(
        functools.partial(kernel, n_tm, n_mom),
        out_shape=(tile, tile),
        in_specs=[
            pl.BlockSpec(memory_space=pltpu.SMEM),
            pl.BlockSpec(memory_space=pltpu.SMEM),
            pl.BlockSpec(memory_space=pltpu.HBM),
        ],
        out_specs=(pl.BlockSpec(memory_space=pltpu.VMEM), pl.BlockSpec(memory_space=pltpu.VMEM)),
        scratch_shapes=scratch,
        compiler_params=pltpu.CompilerParams(
            collective_id=0, has_side_effects=True, vmem_limit_bytes=67_043_328
        ),
    )(mom_pairs.T, deltas, fields)

    return (local.transpose(1, 2, 0)[None], total.transpose(1, 2, 0))


def solution(mesh):
    return jax.shard_map(
        functools.partial(per_device, mesh.shape["tm"], mesh.shape["mom"]),
        mesh=mesh,
        in_specs=(P("tm", "mom", None, None, None), P("mom", None), P()),
        out_specs=(P("tm", None, None, "mom"), P(None, None, "mom")),
        check_vma=False,
    )
```
